256 devices in a mesh: row: 128 (over y, x, z), col: 2 (over core).
Axes of the slice: x: 4, y: 4, z: 8, core: 2. Of those that a mesh axis runs over, the one named last changes fastest.
Arguments:
- features: float32 [64, 32768], P(None, ('row', 'col')), may hold values from -12 to 12
- initial: float32 [32768], P(('row', 'col')), may hold values from 0.1 to 90, as said below
Outputs:
- dist: float32 [32768], P(('row', 'col'))
- residuals: float32 [2], replicated
The draws below stay inside these ranges and needn't reach their ends.
Inputs may be any that keep to these rules, and one draw needn't show every extreme that they name: `initial`: positive starting weights of the policies.
All inputs are finite; a program needn't handle non-finite values.
Results may differ from the reference program's by a relative error of at most 0.0003.
Values sent between devices are 32-bit elements; how exact they have to be, the bound alone decides.
No kernel may reach another device: no remote copies, remote signals or barrier semaphores. Data moves between devices by JAX's collectives and lax.ppermute only.
A program may use at most 64 MiB of HBM per device.

```python
import math
import jax
import jax.numpy as jnp
from jax import lax

NPOL = 32768
FEAT = 64
ITERS = 2


def draw_features(key, part):
    half_feat = FEAT // 2
    noise_key = jax.random.fold_in(key, 11)
    power_key = jax.random.fold_in(key, 12)
    guard_key = jax.random.fold_in(key, 13)
    noise = jnp.clip(0.5 * jax.random.normal(noise_key, (FEAT, NPOL), jnp.float32), -3.0, 3.0)
    strength = jnp.clip(4.0 * jax.random.normal(power_key, (1, NPOL), jnp.float32), -12.0, 12.0)
    guard = jax.random.uniform(guard_key, (1, NPOL), jnp.float32, 0.75, 1.25)
    return jnp.concatenate([strength, noise[1:half_feat], guard, noise[half_feat + 1:]], axis=0)


def draw_initial(key, part):
    base = jnp.exp(jax.random.uniform(key, (NPOL,), jnp.float32, math.log(0.1), math.log(10.0)))
    ramp = 1.0 + 2.0 * jnp.arange(NPOL, dtype=jnp.float32) / NPOL
    return base * ramp


def setup_inputs(seed: int = 0) -> dict:
    streams_of = jax.random.split(jax.random.key(seed), 3)
    return {
        "features": draw_features(jax.random.fold_in(streams_of[2], 71), 0),
        "initial": draw_initial(jax.random.fold_in(streams_of[2], 71), 0),
    }


intensity = 0.25


def reference(features, initial):
    half_feat = FEAT // 2
    row_side_all = jnp.concatenate([features[half_feat:], -features[:half_feat]], axis=0)
    height = min(512, NPOL)
    row_blocks = NPOL // height
    step_rate = 1.0 / NPOL

    def sweep(weights):
        def one_rows(running, block_index):
            offset = (block_index * height).astype(jnp.int32)
            row_side = lax.dynamic_slice_in_dim(row_side_all, offset, height, 1)
            row_mass = lax.dynamic_slice_in_dim(weights, offset, height, 0)
            payoff = jnp.einsum("kr,kc->rc", row_side, features, precision=lax.Precision.HIGHEST)
            moves = jax.nn.sigmoid(intensity * payoff)
            inflow = jnp.dot(row_mass, moves, precision=lax.Precision.HIGHEST)
            return running + inflow, jnp.sum(moves, axis=1)

        inflow, totals = lax.scan(one_rows, jnp.zeros((NPOL,), jnp.float32), jnp.arange(row_blocks, dtype=jnp.int32))
        return inflow, totals.reshape(NPOL)

    weights = initial / jnp.sum(initial)
    changes = []
    for iteration in range(ITERS):
        inflow, totals = sweep(weights)
        advanced = step_rate * inflow + weights * (1.0 - step_rate * totals)
        normalizer = jnp.sum(advanced)
        updated = advanced / normalizer
        changes.append(jnp.sum(jnp.abs(updated - weights)))
        weights = updated
    return NPOL * weights, jnp.stack(changes)
```

```python
import jax
import jax.numpy as jnp
from jax import lax
from jax.experimental import pallas as pl
from jax.experimental.pallas import tpu as pltpu
from jax.sharding import Mesh
from jax.sharding import PartitionSpec as P

NPOL = 32768
AXES = ("row_0", "row_1", "row_2", "col")
PLANE = ("row_0", "row_1")
LINE = ("row_2", "col")
HALF = 32
FEATS = 64
SLOT = 72
LANES = 128
GROUP = 16
BLOCK = GROUP * LANES
STEP = 1.0 / NPOL
SCALE = 0.125

VMEM = pl.BlockSpec(memory_space=pltpu.VMEM)


def halves(x):
    high = x.astype(jnp.bfloat16).astype(jnp.float32)
    return high, x - high


def first_pass(rows_ref, cols_ref, out_ref, t_ref, lhs, rhs, mass):
    total = jnp.zeros((1, LANES), jnp.float32)
    for g in range(GROUP):
        x = rows_ref[g]
        a, b = x[:HALF] * SCALE, x[HALF:FEATS] * SCALE
        high, low = halves(jnp.concatenate([b, -a], axis=0))
        at = pl.ds(g * LANES, LANES)
        lhs[at, 0:LANES] = jnp.concatenate([high, high], axis=0).T.astype(jnp.bfloat16)
        lhs[at, LANES : 2 * LANES] = jnp.concatenate([low, low], axis=0).T.astype(jnp.bfloat16)
        u = x[FEATS : FEATS + 1]
        total += u
        mass[at, :] = jnp.broadcast_to(u, (LANES, LANES)).T
        high, low = halves(cols_ref[g, :FEATS])
        high, low = high.astype(jnp.bfloat16), low.astype(jnp.bfloat16)
        rhs[:, at] = jnp.concatenate([high, low, high, low], axis=0)
    here = jnp.sum(total)

    width = 2 * LANES
    height = 2 * LANES
    for jt in range(BLOCK // width):
        at = pl.ds(jt * width, width)
        right = rhs[:, at]
        flow = jnp.zeros((8, width), jnp.float32)
        plain = jnp.zeros((8, width), jnp.float32)
        for ic in range(BLOCK // height):
            down = pl.ds(ic * height, height)
            t = jnp.tanh(jnp.dot(lhs[down, :], right, preferred_element_type=jnp.float32))
            t_ref[down, at] = t
            m = mass[down, :]
            weighted = t * jnp.concatenate([m, m], axis=1)
            flow += weighted.reshape(height // 8, 8, width).sum(axis=0)
            plain += t.reshape(height // 8, 8, width).sum(axis=0)
        flow = 0.5 * (here + jnp.sum(flow, axis=0, keepdims=True))
        plain = 0.5 * (BLOCK - jnp.sum(plain, axis=0, keepdims=True))
        for k in range(2):
            lane = slice(k * LANES, (k + 1) * LANES)
            for copy in range(GROUP):
                out_ref[copy, pl.ds(2 * jt + k, 1), :] = flow[:, lane]
                out_ref[copy, pl.ds(GROUP + 2 * jt + k, 1), :] = plain[:, lane]


def second_pass(got_ref, cols_ref, t_ref, out_ref, own_ref, u1_ref, sums):
    both = jnp.sum(got_ref[...], axis=0)
    flow, totals = both[:GROUP], both[GROUP:]
    u0 = cols_ref[:, FEATS, :]
    stay = 1.0 - STEP * totals
    u1 = STEP * flow + u0 * stay
    here = jnp.sum(u1)
    u1_ref[0] = u1
    u1_ref[1] = stay
    u1_ref[2] = u0
    p = lax.axis_index(PLANE)
    for k in range(3):
        own_ref[pl.ds(k, 1), :] = u1_ref[k, pl.ds(p, 1), :]
    across = [jnp.broadcast_to(u1[g : g + 1], (8, LANES)) for g in range(GROUP)]

    def one(n, carry):
        down = pl.ds(pl.multiple_of(n * 8, 8), 8)
        acc = t_ref[down, 0:LANES] * across[0]
        for g in range(1, GROUP):
            acc += t_ref[down, g * LANES : (g + 1) * LANES] * across[g]
        sums[down, :] = acc
        return carry

    lax.fori_loop(0, BLOCK // 8, one, 0, unroll=8)
    for g in range(GROUP):
        turned = sums[g * LANES : (g + 1) * LANES, :].T
        out_ref[g] = 0.5 * (here - jnp.sum(turned, axis=0, keepdims=True))


def advance(got_ref, own_ref, out_ref):
    flow = jnp.sum(got_ref[...], axis=0)
    u1, stay, u0 = own_ref[0:1], own_ref[1:2], own_ref[2:3]
    u2 = STEP * flow + u1 * stay
    three = jnp.concatenate([u2, u1, u0], axis=0)
    many = jnp.concatenate([three] * 8, axis=0)
    for n in range(out_ref.shape[0] // 24):
        out_ref[pl.ds(n * 24, 24), :] = many


def finish(all_ref, mine_ref, dist_ref, change_ref):
    count = all_ref.shape[0] // 3
    u2 = all_ref[pl.ds(0, count, stride=3), :]
    u1 = all_ref[pl.ds(1, count, stride=3), :]
    u0 = all_ref[pl.ds(2, count, stride=3), :]
    n2, n1, n0 = jnp.sum(u2), jnp.sum(u1), jnp.sum(u0)
    w2, w1, w0 = u2 / n2, u1 / n1, u0 / n0
    first = jnp.sum(jnp.abs(w1 - w0))
    second = jnp.sum(jnp.abs(w2 - w1))
    dist_ref[...] = NPOL * (mine_ref[0:1, :] / n2)
    lane = lax.broadcasted_iota(jnp.int32, (1, LANES), 1)
    change_ref[...] = jnp.where(lane == 0, first, second)


def everyone(array, axes):
    return lax.all_to_all(array, axes, split_axis=0, concat_axis=0, tiled=True)


def on_device(features, initial):
    f32 = jnp.float32
    whole = jnp.concatenate([features, initial[None], jnp.zeros((SLOT - FEATS - 1, LANES), f32)], axis=0)
    copies = jnp.broadcast_to(whole, (GROUP, SLOT, LANES))
    cols = everyone(copies, PLANE)
    rows = everyone(copies, LINE)
    out, t = pl.pallas_call(
        first_pass,
        out_shape=(
            jax.ShapeDtypeStruct((GROUP, 2 * GROUP, LANES), f32),
            pltpu.VMEM((BLOCK, BLOCK), f32),
        ),
        in_specs=[VMEM] * 2,
        out_specs=(VMEM, VMEM),
        scratch_shapes=[
            pltpu.VMEM((BLOCK, 2 * LANES), jnp.bfloat16),
            pltpu.VMEM((2 * LANES, BLOCK), jnp.bfloat16),
            pltpu.VMEM((BLOCK, LANES), f32),
        ],
        compiler_params=pltpu.CompilerParams(vmem_limit_bytes=24 << 20),
        name="first_pass",
    )(rows, cols)
    got = everyone(out, PLANE)
    partial, own = pl.pallas_call(
        second_pass,
        out_shape=(
            jax.ShapeDtypeStruct((GROUP, 1, LANES), f32),
            jax.ShapeDtypeStruct((3, LANES), f32),
        ),
        in_specs=[VMEM] * 3,
        out_specs=(VMEM, VMEM),
        scratch_shapes=[pltpu.VMEM((3, GROUP, LANES), f32), pltpu.VMEM((BLOCK, LANES), f32)],
        compiler_params=pltpu.CompilerParams(vmem_limit_bytes=20 << 20),
        name="second_pass",
    )(got, cols, t)
    flows = everyone(partial, LINE)
    devices = GROUP * GROUP
    three = pl.pallas_call(
        advance,
        out_shape=jax.ShapeDtypeStruct((3 * devices, LANES), f32),
        in_specs=[VMEM] * 2,
        out_specs=VMEM,
        compiler_params=pltpu.CompilerParams(vmem_limit_bytes=4 << 20),
        name="advance",
    )(flows, own)
    spread = everyone(three.reshape(devices, 1, 3 * LANES), AXES)
    dist, change = pl.pallas_call(
        finish,
        out_shape=(jax.ShapeDtypeStruct((1, LANES), f32), jax.ShapeDtypeStruct((1, LANES), f32)),
        in_specs=[VMEM, VMEM],
        out_specs=(VMEM, VMEM),
        compiler_params=pltpu.CompilerParams(vmem_limit_bytes=4 << 20),
        name="finish",
    )(spread.reshape(3 * devices, LANES), three)
    return dist.reshape(LANES), change[0, :2]


def solution(mesh):
    torus = Mesh(mesh.devices.reshape(4, 4, 8, 2), AXES)
    return jax.shard_map(
        on_device,
        mesh=torus,
        in_specs=(P(None, AXES), P(AXES)),
        out_specs=(P(AXES), P()),
        check_vma=False,
    )
```

```python
import jax
import jax.numpy as jnp
from jax import lax
from jax.experimental import pallas as pl
from jax.experimental.pallas import tpu as pltpu
from jax.sharding import Mesh
from jax.sharding import PartitionSpec as P

NPOL = 32768
AXES = ("row_0", "row_1", "row_2", "col")
PLANE = ("row_0", "row_1")
LINE = ("row_2", "col")
HALF = 32
FEATS = 64
SLOT = 72
LANES = 128
GROUP = 16
BLOCK = GROUP * LANES
STEP = 1.0 / NPOL
SCALE = 0.125
XROWS = 2 * GROUP
YROWS = GROUP + 8
ZROWS = 2 * GROUP + 8

VMEM = pl.BlockSpec(memory_space=pltpu.VMEM)


def halves(x):
    high = x.astype(jnp.bfloat16).astype(jnp.float32)
    return high, x - high


def first_pass(rows_ref, cols_ref, out_ref, t_ref, lhs, rhs, mass):
    total = jnp.zeros((1, LANES), jnp.float32)
    for g in range(GROUP):
        x = rows_ref[g]
        a, b = x[:HALF] * SCALE, x[HALF:FEATS] * SCALE
        high, low = halves(jnp.concatenate([b, -a], axis=0))
        at = pl.ds(g * LANES, LANES)
        lhs[at, 0:LANES] = jnp.concatenate([high, high], axis=0).T.astype(jnp.bfloat16)
        lhs[at, LANES : 2 * LANES] = jnp.concatenate([low, low], axis=0).T.astype(jnp.bfloat16)
        u = x[FEATS : FEATS + 1]
        total += u
        mass[at, :] = jnp.broadcast_to(u, (LANES, LANES)).T
        high, low = halves(cols_ref[g, :FEATS])
        high, low = high.astype(jnp.bfloat16), low.astype(jnp.bfloat16)
        rhs[:, at] = jnp.concatenate([high, low, high, low], axis=0)
    here = jnp.sum(total)

    width = 2 * LANES
    height = 2 * LANES
    for jt in range(BLOCK // width):
        at = pl.ds(jt * width, width)
        right = rhs[:, at]
        flow = jnp.zeros((8, width), jnp.float32)
        plain = jnp.zeros((8, width), jnp.float32)
        for ic in range(BLOCK // height):
            down = pl.ds(ic * height, height)
            t = jnp.tanh(jnp.dot(lhs[down, :], right, preferred_element_type=jnp.float32))
            t_ref[down, at] = t
            m = mass[down, :]
            weighted = t * jnp.concatenate([m, m], axis=1)
            flow += weighted.reshape(height // 8, 8, width).sum(axis=0)
            plain += t.reshape(height // 8, 8, width).sum(axis=0)
        flow = 0.5 * (here + jnp.sum(flow, axis=0, keepdims=True))
        plain = 0.5 * (BLOCK - jnp.sum(plain, axis=0, keepdims=True))
        for k in range(2):
            lane = slice(k * LANES, (k + 1) * LANES)
            for copy in range(GROUP):
                out_ref[copy, pl.ds(2 * jt + k, 1), :] = flow[:, lane]
                out_ref[copy, pl.ds(GROUP + 2 * jt + k, 1), :] = plain[:, lane]


def second_pass(got_ref, cols_ref, t_ref, out_ref, keep, sums):
    both = jnp.sum(got_ref[...], axis=0)
    flow, totals = both[:GROUP], both[GROUP:]
    u0 = cols_ref[:, FEATS, :]
    stay = 1.0 - STEP * totals
    u1 = STEP * flow + u0 * stay
    here = jnp.sum(u1)
    start = jnp.sum(u0)
    keep[0] = u1
    keep[1] = stay
    p = lax.axis_index(PLANE)
    tail = jnp.concatenate(
        [
            keep[0, pl.ds(p, 1), :],
            keep[1, pl.ds(p, 1), :],
            jnp.full((1, LANES), here),
            jnp.full((1, LANES), start),
            jnp.zeros((4, LANES), jnp.float32),
        ],
        axis=0,
    )
    for copy in range(GROUP):
        out_ref[copy, pl.ds(GROUP, 8), :] = tail
    across = [jnp.broadcast_to(u1[g : g + 1], (8, LANES)) for g in range(GROUP)]

    def one(n, carry):
        down = pl.ds(pl.multiple_of(n * 8, 8), 8)
        acc = t_ref[down, 0:LANES] * across[0]
        for g in range(1, GROUP):
            acc += t_ref[down, g * LANES : (g + 1) * LANES] * across[g]
        sums[down, :] = acc
        return carry

    lax.fori_loop(0, BLOCK // 8, one, 0, unroll=8)
    for g in range(GROUP):
        turned = sums[g * LANES : (g + 1) * LANES, :].T
        row = 0.5 * (here - jnp.sum(turned, axis=0, keepdims=True))
        for copy in range(GROUP):
            out_ref[copy, pl.ds(g, 1), :] = row


def advance(got_ref, rows_ref, out_ref):
    flow = jnp.sum(got_ref[:, :GROUP, :], axis=0)
    u1 = got_ref[:, GROUP, :]
    stay = got_ref[:, GROUP + 1, :]
    n1 = jnp.sum(got_ref[:, GROUP + 2, :], axis=0, keepdims=True)
    n0 = jnp.sum(got_ref[:, GROUP + 3, :], axis=0, keepdims=True)
    u2 = STEP * flow + u1 * stay
    w1 = u1 / n1
    u0 = rows_ref[:, FEATS, :]
    change = jnp.sum(jnp.abs(w1 - u0 / n0))
    for copy in range(GROUP):
        out_ref[copy, 0:GROUP, :] = u2
        out_ref[copy, GROUP : 2 * GROUP, :] = w1
        out_ref[copy, 2 * GROUP : ZROWS, :] = jnp.full((8, LANES), change)


def finish(all_ref, dist_ref, change_ref):
    p = lax.axis_index(PLANE)
    q = lax.axis_index(LINE)
    u2 = all_ref[:, :GROUP, :]
    w1 = all_ref[:, GROUP : 2 * GROUP, :]
    first = jnp.sum(all_ref[:, 2 * GROUP, :], axis=0, keepdims=True)
    n2 = jnp.sum(u2)
    second = jnp.sum(jnp.abs(u2 / n2 - w1))
    own = all_ref[pl.ds(p, 1), pl.ds(q, 1), :].reshape(1, LANES)
    dist_ref[...] = NPOL * (own / n2)
    lane = lax.broadcasted_iota(jnp.int32, (1, LANES), 1)
    change_ref[...] = jnp.where(lane == 0, first, second)


def everyone(array, axes):
    return lax.all_to_all(array, axes, split_axis=0, concat_axis=0, tiled=True)


def on_device(features, initial):
    f32 = jnp.float32
    whole = jnp.concatenate([features, initial[None], jnp.zeros((SLOT - FEATS - 1, LANES), f32)], axis=0)
    cols = everyone(jnp.broadcast_to(whole, (GROUP, SLOT, LANES)), PLANE)
    rows = lax.all_gather(whole, LINE, axis=0)
    out, t = pl.pallas_call(
        first_pass,
        out_shape=(
            jax.ShapeDtypeStruct((GROUP, XROWS, LANES), f32),
            pltpu.VMEM((BLOCK, BLOCK), f32),
        ),
        in_specs=[VMEM] * 2,
        out_specs=(VMEM, VMEM),
        scratch_shapes=[
            pltpu.VMEM((BLOCK, 2 * LANES), jnp.bfloat16),
            pltpu.VMEM((2 * LANES, BLOCK), jnp.bfloat16),
            pltpu.VMEM((BLOCK, LANES), f32),
        ],
        compiler_params=pltpu.CompilerParams(vmem_limit_bytes=24 << 20),
        name="first_pass",
    )(rows, cols)
    got = everyone(out, PLANE)
    partial = pl.pallas_call(
        second_pass,
        out_shape=jax.ShapeDtypeStruct((GROUP, YROWS, LANES), f32),
        in_specs=[VMEM] * 3,
        out_specs=VMEM,
        scratch_shapes=[pltpu.VMEM((2, GROUP, LANES), f32), pltpu.VMEM((BLOCK, LANES), f32)],
        compiler_params=pltpu.CompilerParams(vmem_limit_bytes=20 << 20),
        name="second_pass",
    )(got, cols, t)
    flows = everyone(partial, LINE)
    after = pl.pallas_call(
        advance,
        out_shape=jax.ShapeDtypeStruct((GROUP, ZROWS, LANES), f32),
        in_specs=[VMEM] * 2,
        out_specs=VMEM,
        compiler_params=pltpu.CompilerParams(vmem_limit_bytes=4 << 20),
        name="advance",
    )(flows, rows)
    spread = everyone(after, PLANE)
    dist, change = pl.pallas_call(
        finish,
        out_shape=(jax.ShapeDtypeStruct((1, LANES), f32), jax.ShapeDtypeStruct((1, LANES), f32)),
        in_specs=[VMEM],
        out_specs=(VMEM, VMEM),
        compiler_params=pltpu.CompilerParams(vmem_limit_bytes=4 << 20),
        name="finish",
    )(spread)
    return dist.reshape(LANES), change[0, :2]


def solution(mesh):
    torus = Mesh(mesh.devices.reshape(4, 4, 8, 2), AXES)
    return jax.shard_map(
        on_device,
        mesh=torus,
        in_specs=(P(None, AXES), P(AXES)),
        out_specs=(P(AXES), P()),
        check_vma=False,
    )
```

```python
import jax
import jax.numpy as jnp
from jax import lax
from jax.experimental import pallas as pl
from jax.experimental.pallas import tpu as pltpu
from jax.sharding import Mesh
from jax.sharding import PartitionSpec as P

NPOL = 32768
AXES = ("row_0", "row_1", "row_2", "col")
PLANE = ("row_0", "row_1")
LINE = ("row_2", "col")
HALF = 32
FEATS = 64
SLOT = 72
LANES = 128
GROUP = 16
BLOCK = GROUP * LANES
STEP = 1.0 / NPOL
SCALE = 0.125
XROWS = GROUP + 1
YROWS = GROUP + 3
ZROWS = 2 * GROUP + 1

VMEM = pl.BlockSpec(memory_space=pltpu.VMEM)


def halves(x):
    high = x.astype(jnp.bfloat16).astype(jnp.float32)
    return high, x - high


def pack(features_ref, initial_ref, whole_ref, copies_ref):
    tail = jnp.concatenate([initial_ref[...], jnp.zeros((SLOT - FEATS - 1, LANES), jnp.float32)], axis=0)
    whole = jnp.concatenate([features_ref[...], tail], axis=0)
    whole_ref[...] = whole
    for copy in range(GROUP):
        copies_ref[copy] = whole


def first_pass(rows_ref, cols_ref, out_ref, t_ref, lhs, rhs, mass):
    total = jnp.zeros((1, LANES), jnp.float32)
    for g in range(GROUP):
        x = rows_ref[g]
        a, b = x[:HALF] * SCALE, x[HALF:FEATS] * SCALE
        high, low = halves(jnp.concatenate([b, -a], axis=0))
        at = pl.ds(g * LANES, LANES)
        turned = jnp.concatenate([high, low], axis=0).T.astype(jnp.bfloat16)
        lhs[at, 0:LANES] = turned
        lhs[at, LANES : 2 * LANES] = turned
        u = x[FEATS : FEATS + 1]
        total += u
        mass[at, :] = jnp.broadcast_to(u, (LANES, LANES)).T
        high, low = halves(cols_ref[g, :FEATS])
        high, low = high.astype(jnp.bfloat16), low.astype(jnp.bfloat16)
        rhs[:, at] = jnp.concatenate([high, high, low, low], axis=0)
    here = jnp.sum(total)

    width = 2 * LANES
    height = 2 * LANES
    for jt in range(BLOCK // width):
        at = pl.ds(jt * width, width)
        right = rhs[:, at]
        flow = jnp.zeros((8, width), jnp.float32)
        plain = jnp.zeros((8, width), jnp.float32)
        for ic in range(BLOCK // height):
            down = pl.ds(ic * height, height)
            t = jnp.tanh(jnp.dot(lhs[down, :], right, preferred_element_type=jnp.float32))
            t_ref[down, at] = t
            m = mass[down, :]
            weighted = t * jnp.concatenate([m, m], axis=1)
            flow += weighted.reshape(height // 8, 8, width).sum(axis=0)
            plain += t.reshape(height // 8, 8, width).sum(axis=0)
        flow = 0.5 * (here + jnp.sum(flow, axis=0, keepdims=True))
        plain = 0.5 * (BLOCK - jnp.sum(plain, axis=0, keepdims=True))
        for k in range(2):
            lane = slice(k * LANES, (k + 1) * LANES)
            block = 2 * jt + k
            gain = STEP * (flow[:, lane] - cols_ref[block, FEATS : FEATS + 1, :] * plain[:, lane])
            for copy in range(GROUP):
                out_ref[pl.ds(XROWS * copy + block, 1), :] = gain
            out_ref[pl.ds(XROWS * block + GROUP, 1), :] = plain[:, lane]


def second_pass(got_ref, cols_ref, t_ref, out_ref, keep, sums):
    u0 = cols_ref[:, FEATS, :]
    u1 = u0
    for g in range(GROUP):
        u1 += got_ref[XROWS * g : XROWS * g + GROUP, :]
    totals = jnp.sum(got_ref[pl.ds(GROUP, GROUP, stride=XROWS), :], axis=0, keepdims=True)
    here = jnp.sum(u1)
    start = jnp.sum(u0)
    keep[...] = u1
    own = keep[pl.ds(lax.axis_index(PLANE), 1), :]
    lane = lax.broadcasted_iota(jnp.int32, (1, LANES), 1)
    tail = jnp.concatenate([own, 1.0 - STEP * totals, jnp.where(lane < FEATS, here, start)], axis=0)
    for copy in range(GROUP):
        out_ref[pl.ds(YROWS * copy + GROUP, 3), :] = tail
    across = [jnp.broadcast_to(u1[g : g + 1], (8, LANES)) for g in range(GROUP)]

    def one(n, carry):
        down = pl.ds(pl.multiple_of(n * 8, 8), 8)
        acc = t_ref[down, 0:LANES] * across[0]
        for g in range(1, GROUP):
            acc += t_ref[down, g * LANES : (g + 1) * LANES] * across[g]
        sums[down, :] = acc
        return carry

    lax.fori_loop(0, BLOCK // 8, one, 0, unroll=8)
    for g in range(GROUP):
        turned = sums[g * LANES : (g + 1) * LANES, :].T
        row = 0.5 * (here - jnp.sum(turned, axis=0, keepdims=True))
        for copy in range(GROUP):
            out_ref[pl.ds(YROWS * copy + g, 1), :] = row


def advance(got_ref, rows_ref, out_ref):
    flow = got_ref[0:GROUP, :]
    for g in range(1, GROUP):
        flow += got_ref[YROWS * g : YROWS * g + GROUP, :]
    u1 = got_ref[pl.ds(GROUP, GROUP, stride=YROWS), :]
    stay = got_ref[pl.ds(GROUP + 1, GROUP, stride=YROWS), :]
    counts = jnp.sum(got_ref[pl.ds(GROUP + 2, GROUP, stride=YROWS), :], axis=0, keepdims=True)
    n1, n0 = counts[:, 0:1], counts[:, FEATS : FEATS + 1]
    u2 = STEP * flow + u1 * stay
    w1 = u1 / n1
    change = jnp.sum(jnp.abs(w1 - rows_ref[:, FEATS, :] / n0))
    last = jnp.full((1, LANES), change)
    for copy in range(GROUP):
        at = ZROWS * copy
        out_ref[at : at + GROUP, :] = u2
        out_ref[at + GROUP : at + 2 * GROUP, :] = w1
        out_ref[at + 2 * GROUP : at + ZROWS, :] = last


def finish(all_ref, dist_ref, change_ref):
    p = lax.axis_index(PLANE)
    q = lax.axis_index(LINE)
    first = jnp.sum(all_ref[pl.ds(2 * GROUP, GROUP, stride=ZROWS), :], axis=0, keepdims=True)
    u2 = [all_ref[ZROWS * g : ZROWS * g + GROUP, :] for g in range(GROUP)]
    n2 = jnp.sum(sum(u2[1:], u2[0]))
    second = jnp.zeros((GROUP, LANES), jnp.float32)
    for g in range(GROUP):
        second += jnp.abs(u2[g] / n2 - all_ref[ZROWS * g + GROUP : ZROWS * g + 2 * GROUP, :])
    dist_ref[...] = NPOL * (all_ref[pl.ds(ZROWS * p + q, 1), :] / n2)
    lane = lax.broadcasted_iota(jnp.int32, (1, 2), 1)
    change_ref[...] = jnp.where(lane == 0, first[:, 0:2], jnp.sum(second))


def everyone(array, axes):
    count, lanes = array.shape
    blocks = array.reshape(GROUP, 1, count // GROUP * lanes)
    return lax.all_to_all(blocks, axes, split_axis=0, concat_axis=0, tiled=True).reshape(count, lanes)


def call(kernel, outs, megabytes, scratch=()):
    return pl.pallas_call(
        kernel,
        out_shape=outs,
        scratch_shapes=scratch,
        compiler_params=pltpu.CompilerParams(vmem_limit_bytes=megabytes << 20),
        name=kernel.__name__,
    )


def on_device(features, initial):
    def shape(*lengths):
        return jax.ShapeDtypeStruct(lengths, jnp.float32)

    whole, copies = call(pack, (shape(SLOT, LANES), shape(GROUP, SLOT, LANES)), 62)(
        features, initial.reshape(1, LANES)
    )
    cols = lax.all_to_all(copies, PLANE, split_axis=0, concat_axis=0, tiled=True)
    rows = lax.all_gather(whole, LINE, axis=0)
    gain, t = call(
        first_pass,
        (shape(GROUP * XROWS, LANES), pltpu.VMEM((BLOCK, BLOCK), jnp.float32)),
        24,
        (
            pltpu.VMEM((BLOCK, 2 * LANES), jnp.bfloat16),
            pltpu.VMEM((2 * LANES, BLOCK), jnp.bfloat16),
            pltpu.VMEM((BLOCK, LANES), jnp.float32),
        ),
    )(rows, cols)
    flow = call(
        second_pass,
        shape(GROUP * YROWS, LANES),
        20,
        (pltpu.VMEM((GROUP, LANES), jnp.float32), pltpu.VMEM((BLOCK, LANES), jnp.float32)),
    )(everyone(gain, PLANE), cols, t)
    after = call(advance, shape(GROUP * ZROWS, LANES), 4)(everyone(flow, LINE), rows)
    dist, change = call(finish, (shape(1, LANES), shape(1, 2)), 4)(everyone(after, PLANE))
    return dist.reshape(LANES), change.reshape(2)


def solution(mesh):
    torus = Mesh(mesh.devices.reshape(4, 4, 8, 2), AXES)
    return jax.shard_map(
        on_device,
        mesh=torus,
        in_specs=(P(None, AXES), P(AXES)),
        out_specs=(P(AXES), P()),
        check_vma=False,
    )
```

```python
import jax
import jax.numpy as jnp
from jax import lax
from jax.experimental import pallas as pl
from jax.experimental.pallas import tpu as pltpu
from jax.sharding import Mesh
from jax.sharding import PartitionSpec as P

NPOL = 32768
AXES = ("row_0", "row_1", "row_2", "col")
PLANE = ("row_0", "row_1")
LINE = ("row_2", "col")
HALF = 32
FEATS = 64
SLOT = 72
LANES = 128
GROUP = 16
BLOCK = GROUP * LANES
STEP = 1.0 / NPOL
SCALE = 0.125
XROWS = GROUP + 1
YROWS = GROUP + 3
ZROWS = 2 * GROUP + 1

VMEM = pl.BlockSpec(memory_space=pltpu.VMEM)


def pieces(x):
    high = x.astype(jnp.bfloat16).astype(jnp.float32)
    middle = (x - high).astype(jnp.bfloat16).astype(jnp.float32)
    return high, middle, (x - high) - middle


def pack(features_ref, initial_ref, whole_ref, copies_ref):
    tail = jnp.concatenate([initial_ref[...], jnp.zeros((SLOT - FEATS - 1, LANES), jnp.float32)], axis=0)
    whole = jnp.concatenate([features_ref[...], tail], axis=0)
    whole_ref[...] = whole
    for copy in range(GROUP):
        copies_ref[copy] = whole


def first_pass(rows_ref, cols_ref, out_ref, t_ref, lhs, rhs, mass):
    total = jnp.zeros((1, LANES), jnp.float32)
    for g in range(GROUP):
        x = rows_ref[g]
        a, b = x[:HALF] * SCALE, x[HALF:FEATS] * SCALE
        high, middle, low = pieces(jnp.concatenate([b, -a], axis=0))
        at = pl.ds(g * LANES, LANES)
        turned = jnp.concatenate([high, middle], axis=0).T.astype(jnp.bfloat16)
        lhs[at, 0:LANES] = turned
        lhs[at, LANES : 2 * LANES] = turned
        lhs[at, 2 * LANES : 3 * LANES] = jnp.concatenate([high, low], axis=0).T.astype(jnp.bfloat16)
        u = x[FEATS : FEATS + 1]
        total += u
        mass[at, :] = jnp.broadcast_to(u, (LANES, LANES)).T
        high, middle, low = (y.astype(jnp.bfloat16) for y in pieces(cols_ref[g, :FEATS]))
        rhs[:, at] = jnp.concatenate([high, high, middle, middle, low, high], axis=0)
    here = jnp.sum(total)

    width = 2 * LANES
    height = 2 * LANES
    for jt in range(BLOCK // width):
        at = pl.ds(jt * width, width)
        right = rhs[:, at]
        flow = jnp.zeros((8, width), jnp.float32)
        plain = jnp.zeros((8, width), jnp.float32)
        for ic in range(BLOCK // height):
            down = pl.ds(ic * height, height)
            t = jnp.tanh(jnp.dot(lhs[down, :], right, preferred_element_type=jnp.float32))
            t_ref[down, at] = t
            m = mass[down, :]
            weighted = t * jnp.concatenate([m, m], axis=1)
            flow += weighted.reshape(height // 8, 8, width).sum(axis=0)
            plain += t.reshape(height // 8, 8, width).sum(axis=0)
        flow = 0.5 * (here + jnp.sum(flow, axis=0, keepdims=True))
        plain = 0.5 * (BLOCK - jnp.sum(plain, axis=0, keepdims=True))
        for k in range(2):
            lane = slice(k * LANES, (k + 1) * LANES)
            block = 2 * jt + k
            gain = STEP * (flow[:, lane] - cols_ref[block, FEATS : FEATS + 1, :] * plain[:, lane])
            for copy in range(GROUP):
                out_ref[pl.ds(XROWS * copy + block, 1), :] = gain
            out_ref[pl.ds(XROWS * block + GROUP, 1), :] = plain[:, lane]


def second_pass(got_ref, cols_ref, t_ref, out_ref, keep):
    u0 = cols_ref[:, FEATS, :]
    u1 = u0
    for g in range(GROUP):
        u1 += got_ref[XROWS * g : XROWS * g + GROUP, :]
    totals = jnp.sum(got_ref[pl.ds(GROUP, GROUP, stride=XROWS), :], axis=0, keepdims=True)
    here = jnp.sum(u1)
    start = jnp.sum(u0)
    keep[...] = u1
    own = keep[pl.ds(lax.axis_index(PLANE), 1), :]
    lane = lax.broadcasted_iota(jnp.int32, (1, LANES), 1)
    tail = jnp.concatenate([own, 1.0 - STEP * totals, jnp.where(lane < FEATS, here, start)], axis=0)
    for copy in range(GROUP):
        out_ref[pl.ds(YROWS * copy + GROUP, 3), :] = tail
    across = [jnp.broadcast_to(u1[g : g + 1], (8, LANES)) for g in range(GROUP)]
    for g in range(GROUP):
        parts = []
        for n in range(LANES // 8):
            down = slice(g * LANES + n * 8, g * LANES + n * 8 + 8)
            acc = t_ref[down, 0:LANES] * across[0]
            for k in range(1, GROUP):
                acc += t_ref[down, k * LANES : (k + 1) * LANES] * across[k]
            parts.append(acc)
        turned = jnp.concatenate(parts, axis=0).T
        row = 0.5 * (here - jnp.sum(turned, axis=0, keepdims=True))
        for copy in range(GROUP):
            out_ref[pl.ds(YROWS * copy + g, 1), :] = row


def advance(got_ref, rows_ref, out_ref):
    flow = got_ref[0:GROUP, :]
    for g in range(1, GROUP):
        flow += got_ref[YROWS * g : YROWS * g + GROUP, :]
    u1 = got_ref[pl.ds(GROUP, GROUP, stride=YROWS), :]
    stay = got_ref[pl.ds(GROUP + 1, GROUP, stride=YROWS), :]
    counts = jnp.sum(got_ref[pl.ds(GROUP + 2, GROUP, stride=YROWS), :], axis=0, keepdims=True)
    n1, n0 = counts[:, 0:1], counts[:, FEATS : FEATS + 1]
    u2 = STEP * flow + u1 * stay
    w1 = u1 / n1
    change = jnp.sum(jnp.abs(w1 - rows_ref[:, FEATS, :] / n0))
    last = jnp.full((1, LANES), change)
    for copy in range(GROUP):
        at = ZROWS * copy
        out_ref[at : at + GROUP, :] = u2
        out_ref[at + GROUP : at + 2 * GROUP, :] = w1
        out_ref[at + 2 * GROUP : at + ZROWS, :] = last


def finish(all_ref, dist_ref, change_ref):
    p = lax.axis_index(PLANE)
    q = lax.axis_index(LINE)
    first = jnp.sum(all_ref[pl.ds(2 * GROUP, GROUP, stride=ZROWS), :], axis=0, keepdims=True)
    u2 = [all_ref[ZROWS * g : ZROWS * g + GROUP, :] for g in range(GROUP)]
    n2 = jnp.sum(sum(u2[1:], u2[0]))
    second = jnp.zeros((GROUP, LANES), jnp.float32)
    for g in range(GROUP):
        second += jnp.abs(u2[g] / n2 - all_ref[ZROWS * g + GROUP : ZROWS * g + 2 * GROUP, :])
    dist_ref[...] = NPOL * (all_ref[pl.ds(ZROWS * p + q, 1), :] / n2)
    lane = lax.broadcasted_iota(jnp.int32, (1, 2), 1)
    change_ref[...] = jnp.where(lane == 0, first[:, 0:2], jnp.sum(second))


def everyone(array, axes):
    count, lanes = array.shape
    blocks = array.reshape(GROUP, 1, count // GROUP * lanes)
    return lax.all_to_all(blocks, axes, split_axis=0, concat_axis=0, tiled=True).reshape(count, lanes)


def call(kernel, outs, megabytes, scratch=()):
    return pl.pallas_call(
        kernel,
        out_shape=outs,
        scratch_shapes=scratch,
        compiler_params=pltpu.CompilerParams(vmem_limit_bytes=megabytes << 20),
        name=kernel.__name__,
    )


def on_device(features, initial):
    def shape(*lengths):
        return jax.ShapeDtypeStruct(lengths, jnp.float32)

    whole, copies = call(pack, (shape(SLOT, LANES), shape(GROUP, SLOT, LANES)), 62)(
        features, initial.reshape(1, LANES)
    )
    cols = lax.all_to_all(copies, PLANE, split_axis=0, concat_axis=0, tiled=True)
    rows = lax.all_gather(whole, LINE, axis=0)
    gain, t = call(
        first_pass,
        (shape(GROUP * XROWS, LANES), pltpu.VMEM((BLOCK, BLOCK), jnp.float32)),
        24,
        (
            pltpu.VMEM((BLOCK, 3 * LANES), jnp.bfloat16),
            pltpu.VMEM((3 * LANES, BLOCK), jnp.bfloat16),
            pltpu.VMEM((BLOCK, LANES), jnp.float32),
        ),
    )(rows, cols)
    flow = call(
        second_pass,
        shape(GROUP * YROWS, LANES),
        20,
        (pltpu.VMEM((GROUP, LANES), jnp.float32),),
    )(everyone(gain, PLANE), cols, t)
    after = call(advance, shape(GROUP * ZROWS, LANES), 4)(everyone(flow, LINE), rows)
    dist, change = call(finish, (shape(1, LANES), shape(1, 2)), 4)(everyone(after, PLANE))
    return dist.reshape(LANES), change.reshape(2)


def solution(mesh):
    torus = Mesh(mesh.devices.reshape(4, 4, 8, 2), AXES)
    return jax.shard_map(
        on_device,
        mesh=torus,
        in_specs=(P(None, AXES), P(AXES)),
        out_specs=(P(AXES), P()),
        check_vma=False,
    )
```

```python
import jax
import jax.numpy as jnp
from jax import lax
from jax.experimental import pallas as pl
from jax.experimental.pallas import tpu as pltpu
from jax.sharding import Mesh
from jax.sharding import PartitionSpec as P

NPOL = 32768
AXES = ("row_0", "row_1", "row_2", "col")
PLANE = ("row_0", "row_1")
LINE = ("row_2", "col")
HALF = 32
FEATS = 64
SLOT = 72
LANES = 128
GROUP = 16
BLOCK = GROUP * LANES
STEP = 1.0 / NPOL
SCALE = 0.125
XROWS = GROUP + 1
CHIPS = GROUP // 2
YROWS = GROUP + 5
ZROWS = 2 * GROUP + 1

VMEM = pl.BlockSpec(memory_space=pltpu.VMEM)


def pieces(x):
    high = x.astype(jnp.bfloat16).astype(jnp.float32)
    middle = (x - high).astype(jnp.bfloat16).astype(jnp.float32)
    return high, middle, (x - high) - middle


def pack(features_ref, initial_ref, whole_ref, copies_ref):
    tail = jnp.concatenate([initial_ref[...], jnp.zeros((SLOT - FEATS - 1, LANES), jnp.float32)], axis=0)
    whole = jnp.concatenate([features_ref[...], tail], axis=0)
    whole_ref[...] = whole
    for copy in range(GROUP):
        copies_ref[copy] = whole


def first_pass(rows_ref, cols_ref, out_ref, t_ref, lhs, rhs, mass):
    total = jnp.zeros((1, LANES), jnp.float32)
    for g in range(GROUP):
        x = rows_ref[g]
        a, b = x[:HALF] * SCALE, x[HALF:FEATS] * SCALE
        high, middle, low = pieces(jnp.concatenate([b, -a], axis=0))
        at = pl.ds(g * LANES, LANES)
        turned = jnp.concatenate([high, middle], axis=0).T.astype(jnp.bfloat16)
        lhs[at, 0:LANES] = turned
        lhs[at, LANES : 2 * LANES] = turned
        lhs[at, 2 * LANES : 3 * LANES] = jnp.concatenate([high, low], axis=0).T.astype(jnp.bfloat16)
        u = x[FEATS : FEATS + 1]
        total += u
        mass[at, :] = jnp.broadcast_to(u, (LANES, LANES)).T
        high, middle, low = (y.astype(jnp.bfloat16) for y in pieces(cols_ref[g, :FEATS]))
        rhs[:, at] = jnp.concatenate([high, high, middle, middle, low, high], axis=0)
    here = jnp.sum(total)

    width = 2 * LANES
    height = 2 * LANES
    for jt in range(BLOCK // width):
        at = pl.ds(jt * width, width)
        right = rhs[:, at]
        flow = jnp.zeros((8, width), jnp.float32)
        plain = jnp.zeros((8, width), jnp.float32)
        for ic in range(BLOCK // height):
            down = pl.ds(ic * height, height)
            t = jnp.tanh(jnp.dot(lhs[down, :], right, preferred_element_type=jnp.float32))
            t_ref[down, at] = t
            m = mass[down, :]
            weighted = t * jnp.concatenate([m, m], axis=1)
            flow += weighted.reshape(height // 8, 8, width).sum(axis=0)
            plain += t.reshape(height // 8, 8, width).sum(axis=0)
        flow = 0.5 * (here + jnp.sum(flow, axis=0, keepdims=True))
        plain = 0.5 * (BLOCK - jnp.sum(plain, axis=0, keepdims=True))
        for k in range(2):
            lane = slice(k * LANES, (k + 1) * LANES)
            block = 2 * jt + k
            gain = STEP * (flow[:, lane] - cols_ref[block, FEATS : FEATS + 1, :] * plain[:, lane])
            for copy in range(GROUP):
                out_ref[pl.ds(XROWS * copy + block, 1), :] = gain
            out_ref[pl.ds(XROWS * block + GROUP, 1), :] = plain[:, lane]


def second_pass(got_ref, cols_ref, t_ref, out_ref, keep):
    u0 = cols_ref[:, FEATS, :]
    u1 = u0
    for g in range(GROUP):
        u1 += got_ref[XROWS * g : XROWS * g + GROUP, :]
    totals = jnp.sum(got_ref[pl.ds(GROUP, GROUP, stride=XROWS), :], axis=0, keepdims=True)
    here = jnp.sum(u1)
    start = jnp.sum(u0)
    keep[...] = u1
    own = keep[pl.ds(lax.axis_index(PLANE), 1), :]
    lane = lax.broadcasted_iota(jnp.int32, (1, LANES), 1)
    tail = jnp.concatenate([own, 1.0 - STEP * totals, jnp.where(lane < FEATS, here, start)], axis=0)
    out_ref[GROUP : GROUP + 3, :] = tail
    across = [jnp.broadcast_to(u1[g : g + 1], (8, LANES)) for g in range(GROUP)]
    for g in range(GROUP):
        parts = []
        for n in range(LANES // 8):
            down = slice(g * LANES + n * 8, g * LANES + n * 8 + 8)
            acc = t_ref[down, 0:LANES] * across[0]
            for k in range(1, GROUP):
                acc += t_ref[down, k * LANES : (k + 1) * LANES] * across[k]
            parts.append(acc)
        turned = jnp.concatenate(parts, axis=0).T
        row = 0.5 * (here - jnp.sum(turned, axis=0, keepdims=True))
        at = g % 2 * CHIPS + g // 2
        out_ref[at : at + 1, :] = row


def join(mine_ref, other_ref, out_ref):
    zero = lax.axis_index("col") == 0
    mine, other = mine_ref[GROUP : GROUP + 3, :], other_ref[GROUP : GROUP + 3, :]
    even, odd = jnp.where(zero, mine, other), jnp.where(zero, other, mine)
    flow = mine_ref[0:GROUP, :] + other_ref[0:GROUP, :]
    tail = jnp.concatenate([even[0:1], odd[0:1], even[1:2], odd[1:2], mine[2:3] + other[2:3]], axis=0)
    for copy in range(CHIPS):
        at = YROWS * copy
        out_ref[at : at + GROUP, :] = flow
        out_ref[at + GROUP : at + YROWS, :] = tail


def advance(got_ref, rows_ref, out_ref):
    def every(row):
        return got_ref[pl.ds(row, CHIPS, stride=YROWS), :]

    flow = got_ref[0:GROUP, :]
    for k in range(1, CHIPS):
        flow += got_ref[YROWS * k : YROWS * k + GROUP, :]
    u1 = jnp.concatenate([every(GROUP), every(GROUP + 1)], axis=0)
    stay = jnp.concatenate([every(GROUP + 2), every(GROUP + 3)], axis=0)
    counts = jnp.sum(every(GROUP + 4), axis=0, keepdims=True)
    n1, n0 = counts[:, 0:1], counts[:, FEATS : FEATS + 1]
    u0 = jnp.concatenate(
        [rows_ref[2 * k + c, FEATS : FEATS + 1, :] for c in range(2) for k in range(CHIPS)], axis=0
    )
    u2 = STEP * flow + u1 * stay
    w1 = u1 / n1
    change = jnp.sum(jnp.abs(w1 - u0 / n0))
    last = jnp.full((1, LANES), change)
    for copy in range(GROUP):
        at = ZROWS * copy
        out_ref[at : at + GROUP, :] = u2
        out_ref[at + GROUP : at + 2 * GROUP, :] = w1
        out_ref[at + 2 * GROUP : at + ZROWS, :] = last


def finish(all_ref, dist_ref, change_ref):
    p = lax.axis_index(PLANE)
    q = CHIPS * lax.axis_index("col") + lax.axis_index("row_2")
    first = jnp.sum(all_ref[pl.ds(2 * GROUP, GROUP, stride=ZROWS), :], axis=0, keepdims=True)
    u2 = [all_ref[ZROWS * g : ZROWS * g + GROUP, :] for g in range(GROUP)]
    n2 = jnp.sum(sum(u2[1:], u2[0]))
    second = jnp.zeros((GROUP, LANES), jnp.float32)
    for g in range(GROUP):
        second += jnp.abs(u2[g] / n2 - all_ref[ZROWS * g + GROUP : ZROWS * g + 2 * GROUP, :])
    dist_ref[...] = NPOL * (all_ref[pl.ds(ZROWS * p + q, 1), :] / n2)
    lane = lax.broadcasted_iota(jnp.int32, (1, 2), 1)
    change_ref[...] = jnp.where(lane == 0, first[:, 0:2], jnp.sum(second))


def everyone(array, axes):
    count, lanes = array.shape
    members = lax.axis_size(axes)
    blocks = array.reshape(members, 1, count // members * lanes)
    return lax.all_to_all(blocks, axes, split_axis=0, concat_axis=0, tiled=True).reshape(count, lanes)


def call(kernel, outs, megabytes, scratch=()):
    return pl.pallas_call(
        kernel,
        out_shape=outs,
        scratch_shapes=scratch,
        compiler_params=pltpu.CompilerParams(vmem_limit_bytes=megabytes << 20),
        name=kernel.__name__,
    )


def on_device(features, initial):
    def shape(*lengths):
        return jax.ShapeDtypeStruct(lengths, jnp.float32)

    whole, copies = call(pack, (shape(SLOT, LANES), shape(GROUP, SLOT, LANES)), 62)(
        features, initial.reshape(1, LANES)
    )
    cols = lax.all_to_all(copies, PLANE, split_axis=0, concat_axis=0, tiled=True)
    rows = lax.all_gather(whole, LINE, axis=0)
    gain, t = call(
        first_pass,
        (shape(GROUP * XROWS, LANES), pltpu.VMEM((BLOCK, BLOCK), jnp.float32)),
        24,
        (
            pltpu.VMEM((BLOCK, 3 * LANES), jnp.bfloat16),
            pltpu.VMEM((3 * LANES, BLOCK), jnp.bfloat16),
            pltpu.VMEM((BLOCK, LANES), jnp.float32),
        ),
    )(rows, cols)
    flow = call(
        second_pass,
        shape(GROUP + 3, LANES),
        20,
        (pltpu.VMEM((GROUP, LANES), jnp.float32),),
    )(everyone(gain, PLANE), cols, t)
    other = lax.ppermute(flow, "col", [(0, 1), (1, 0)])
    both = call(join, shape(CHIPS * YROWS, LANES), 4)(flow, other)
    after = call(advance, shape(GROUP * ZROWS, LANES), 4)(everyone(both, "row_2"), rows)
    dist, change = call(finish, (shape(1, LANES), shape(1, 2)), 4)(everyone(after, PLANE))
    return dist.reshape(LANES), change.reshape(2)


def solution(mesh):
    torus = Mesh(mesh.devices.reshape(4, 4, 8, 2), AXES)
    return jax.shard_map(
        on_device,
        mesh=torus,
        in_specs=(P(None, AXES), P(AXES)),
        out_specs=(P(AXES), P()),
        check_vma=False,
    )
```
